256 devices in a mesh: parts: 2 (over z), uly: 8 (over x), blk: 16 (over y, core).
Axes of the slice: x: 8, y: 8, z: 2, core: 2. Of those that a mesh axis runs over, the one named last changes fastest.
The devices are a block of a 8x8x16 slice.
Arguments:
- queries: bfloat16 [32, 512, 8192], P(('parts', 'blk'), 'uly'), parts along dimension 0, may hold values from -4.5 to 4.5
- keys: bfloat16 [32, 512, 1024], P(('parts', 'blk'), 'uly'), parts along dimension 0, may hold values from -4.5 to 4.5
- values: bfloat16 [32, 512, 1024], P(('parts', 'blk'), 'uly'), parts along dimension 0, may hold values from -6 to 6
- doc_blocks: int32 [32], P('parts'), parts along dimension 0, may hold values from 1 to 36, 64 in all
Outputs:
- attended: bfloat16 [32, 512, 8192], P(('parts', 'blk'), 'uly'), parts along dimension 0
The draws below stay inside these ranges and needn't reach their ends.
There are 2 independent parts, one for each index of `parts`. The reference program is written for one: setup_inputs(seed, part) draws one part's arguments, and reference() takes and returns one part's arrays. A program takes and returns all parts, laid end to end along the dimension named above; each array names one. Nothing has to cross between parts.
Inputs may be any that keep to these rules, and one draw needn't show every extreme that they name: `doc_blocks`: the lengths sum to 64; the longest document holds exactly (9) * 512 tokens.
All inputs are finite; a program needn't handle non-finite values.
Results may differ from the reference program's by a relative error of at most 0.0037.
Values may be sent and summed in bfloat16 or wider, within the bound.
No kernel may reach another device: no remote copies, remote signals or barrier semaphores. Data moves between devices by JAX's collectives and lax.ppermute only.
A program may use at most 128 MiB of HBM per device.

```python
import math
import jax
import jax.numpy as jnp
import numpy as np
from jax import lax

QUERY_HEADS = 64
KEY_VALUE_HEADS = 8
HEAD_WIDTH = 128
BLOCK = 128
BLOCK_TOKENS = 512
DOCS = 16
N_BLK = 16


def draw_queries(key, part):
    total_count = N_BLK * BLOCK_TOKENS
    query_group = QUERY_HEADS // KEY_VALUE_HEADS
    fresh_state = jax.random.fold_in(key, 11)
    base_offset = jnp.clip(jax.random.normal(fresh_state, (total_count, KEY_VALUE_HEADS, query_group, HEAD_WIDTH), jnp.float32), -4.5, 4.5)
    return base_offset.reshape(N_BLK, BLOCK_TOKENS, QUERY_HEADS * HEAD_WIDTH).astype(jnp.bfloat16)


def draw_keys(key, part):
    total_count = N_BLK * BLOCK_TOKENS
    fresh_state = jax.random.fold_in(key, 13)
    base_offset = jnp.clip(jax.random.normal(fresh_state, (total_count, KEY_VALUE_HEADS, HEAD_WIDTH), jnp.float32), -4.5, 4.5)
    return base_offset.reshape(N_BLK, BLOCK_TOKENS, KEY_VALUE_HEADS * HEAD_WIDTH).astype(jnp.bfloat16)


def block_scale(own_key, dims, cuts, smallest, top_value):
    level, own = 1.0, jax.random.fold_in(own_key, 6)
    for dim, shards_of in cuts:
        steps = jnp.exp(jax.random.uniform(jax.random.fold_in(own, dim), (shards_of,), jnp.float32, smallest / len(cuts), top_value / len(cuts)))
        level = level * jnp.repeat(steps, dims[dim] // shards_of).reshape([-1 if axis == dim else 1 for axis in range(len(dims))])
    return level


def length_profile(amount, total, limit, lean):
    weights = [(1 << 20) // math.isqrt(grade ** lean) + 1 for grade in range(2, amount + 1)]
    spare, counts = total - limit - (amount - 1), [1] * (amount - 1)
    while spare > 0:
        candidates = [i for i in range(amount - 1) if counts[i] < limit]
        pool, left = sum([weights[i] for i in candidates]), spare
        for i in candidates:
            extra = min(limit - counts[i], max(1, left * weights[i] // pool), spare)
            counts[i] = counts[i] + extra
            spare = spare - extra
    return np.array([limit] + counts)


def uneven_parts(own_key, amount, total, limit, skew):
    if amount == 2:
        one = jax.random.randint(own_key, (), max(1, total - limit), min(limit, total - 1) + 1)
        return jnp.stack([one, total - one])
    lengths = jnp.asarray(length_profile(amount, total, limit, skew), jnp.int32)
    twos = (amount - 1) // 2
    donor, receiver = lengths[1:1 + 2 * twos:2], lengths[2:2 + 2 * twos:2]
    margin = jnp.minimum(donor - 1, limit - receiver)
    shifted = jax.random.randint(jax.random.fold_in(own_key, 1), (twos,), 0, 1 << 20) % (margin + 1)
    lengths = lengths.at[1:1 + 2 * twos:2].set(donor - shifted).at[2:2 + 2 * twos:2].set(receiver + shifted)
    return lengths[jax.random.permutation(jax.random.fold_in(own_key, 2), amount)]


def gaussian(own_key, dims, scale, reach, cuts=(), kind=jnp.bfloat16):
    values = jax.random.normal(own_key, dims, jnp.float32) * scale
    if len(cuts) > 0:
        values = block_scale(own_key, dims, cuts, -0.22, 0.18) * values
    return jnp.clip(values, min=-reach, max=reach).astype(kind)


def setup_inputs(seed: int = 0, part: int = 0) -> dict:
    seeds = jax.random.split(jax.random.key(seed), 5)
    part_keys = jax.random.split(jax.random.fold_in(seeds[4], part), 5)
    return {
        "queries": draw_queries(jax.random.fold_in(jax.random.fold_in(seeds[4], part), 71), part),
        "keys": draw_keys(jax.random.fold_in(jax.random.fold_in(seeds[4], part), 71), part),
        "values": gaussian(part_keys[2], (N_BLK, BLOCK_TOKENS, KEY_VALUE_HEADS * HEAD_WIDTH), 1.0, 6.0, ((0, 16), (1, 8))),
        "doc_blocks": uneven_parts(part_keys[3], DOCS, N_BLK * BLOCK_TOKENS // BLOCK, (N_BLK // 2 + 1) * BLOCK_TOKENS // BLOCK, 2).astype(jnp.int32),
    }


def reference(queries, keys, values, doc_blocks):
    total_count = N_BLK * BLOCK_TOKENS
    query_group = QUERY_HEADS // KEY_VALUE_HEADS
    scale = HEAD_WIDTH ** -0.5
    q = queries.reshape(N_BLK, BLOCK_TOKENS, KEY_VALUE_HEADS, query_group, HEAD_WIDTH)
    key_rows = keys.reshape(N_BLK, BLOCK_TOKENS, KEY_VALUE_HEADS, HEAD_WIDTH)
    value_rows = values.reshape(N_BLK, BLOCK_TOKENS, KEY_VALUE_HEADS, HEAD_WIDTH)
    ends = jnp.cumsum(doc_blocks).astype(jnp.int32) * BLOCK
    pos = jnp.arange(total_count, dtype=jnp.int32)
    seg = jnp.sum((pos[:, None] >= ends[None, :]).astype(jnp.int32), axis=1).astype(jnp.int32)
    seg = seg.reshape(N_BLK, BLOCK_TOKENS)
    first_seg = seg[:, 0]
    last_seg = seg[:, -1]

    def one_slot(index):
        qs = lax.dynamic_index_in_dim(q, index, 0, keepdims=False).astype(jnp.float32)
        qseg = lax.dynamic_index_in_dim(seg, index, 0, keepdims=False)
        qpos = index * BLOCK_TOKENS + jnp.arange(BLOCK_TOKENS, dtype=jnp.int32)
        qfirst = lax.dynamic_index_in_dim(first_seg, index, 0, keepdims=False)

        def scores_of(other):
            ks = lax.dynamic_index_in_dim(key_rows, other, 0, keepdims=False).astype(jnp.float32)
            kseg = lax.dynamic_index_in_dim(seg, other, 0, keepdims=False)
            kpos = other * BLOCK_TOKENS + jnp.arange(BLOCK_TOKENS, dtype=jnp.int32)
            allowed = (qseg[:, None] == kseg[None, :]) & (kpos[None, :] <= qpos[:, None])
            scores = jnp.einsum('tghd,sgd->ghts', qs, ks) * scale
            return allowed, jnp.where(allowed[None, None], scores, -1e30)

        def useful(other):
            klast = lax.dynamic_index_in_dim(last_seg, other, 0, keepdims=False)
            return (other <= index) & (klast >= qfirst)

        def max_step(most, other):
            def work(current):
                return jnp.maximum(current, jnp.max(scores_of(other)[1], axis=-1))
            return lax.cond(useful(other), work, lambda current: current, most), None

        start_most = jnp.full((KEY_VALUE_HEADS, query_group, BLOCK_TOKENS), -1e30, jnp.float32)
        most, unused = lax.scan(max_step, start_most, jnp.arange(N_BLK, dtype=jnp.int32))

        def sum_step(carry, other):
            def work(state):
                total, accum = state
                allowed, scores = scores_of(other)
                expo = jnp.where(allowed[None, None], jnp.exp(scores - most[..., None]), 0.0)
                weights = expo.astype(jnp.bfloat16).astype(jnp.float32)
                vs = lax.dynamic_index_in_dim(value_rows, other, 0, keepdims=False).astype(jnp.float32)
                return total + jnp.sum(expo, axis=-1), accum + jnp.einsum('ghts,sgd->ghtd', weights, vs)
            return lax.cond(useful(other), work, lambda state: state, carry), None

        start_state = (jnp.zeros((KEY_VALUE_HEADS, query_group, BLOCK_TOKENS), jnp.float32), jnp.zeros((KEY_VALUE_HEADS, query_group, BLOCK_TOKENS, HEAD_WIDTH), jnp.float32))
        (total, accum), unused = lax.scan(sum_step, start_state, jnp.arange(N_BLK, dtype=jnp.int32))
        out = (accum / total[..., None]).astype(jnp.bfloat16)
        return jnp.transpose(out, (2, 0, 1, 3)).reshape(BLOCK_TOKENS, QUERY_HEADS * HEAD_WIDTH)

    return lax.map(one_slot, jnp.arange(N_BLK, dtype=jnp.int32))
```

```python
import jax
import jax.numpy as jnp
from jax import lax
from jax.experimental import pallas as pl
from jax.experimental.pallas import tpu as pltpu
from jax.sharding import Mesh, PartitionSpec as P

HEAD_WIDTH = 128
BLOCK = 128
CORES = 2
TILE = 512
LOG2E = 1.4426950408889634
SCALE = LOG2E * HEAD_WIDTH ** -0.5


def attention(where, docs, q, pieces):
    blocks, chunk, wide = q.shape
    heads = wide // HEAD_WIDTH
    rows = heads * chunk
    arrays = [p[0] for p in pieces]
    n = len(arrays)
    n_x = n // CORES
    block_tokens = n_x * chunk
    total = blocks * CORES * block_tokens
    n_docs = docs.shape[0]
    places = where

    def kernel(place, doc, q_ref, *refs):
        srcs, (o_ref, k_all, v_all, m_ref, l_ref, a_ref, sems) = refs[:n], refs[n:]
        step = pl.program_id(0)

        def copies():
            for i in range(n):
                at = place[2 + 2 * i]
                core = place[3 + 2 * i]
                for kind, dst in ((0, k_all), (1, v_all)):
                    yield pltpu.make_async_copy(
                        srcs[i].at[:, kind], dst.at[pl.ds(0, blocks), core, at], sems.at[kind, i]
                    )

        @pl.when(step == 0)
        def _():
            for c in copies():
                c.start()
            k_all[blocks, 0] = jnp.zeros((n_x, chunk, HEAD_WIDTH), jnp.bfloat16)
            v_all[blocks, 0] = jnp.zeros((n_x, chunk, HEAD_WIDTH), jnp.bfloat16)
            for c in copies():
                c.wait()

        first = (step * CORES + place[1]) * block_tokens + place[0] * chunk
        begin = jnp.int32(0)
        end = jnp.int32(0)
        for i in range(n_docs):
            end = end + doc[i] * BLOCK
            begin = jnp.where(end <= first, end, begin)
        span = first + chunk - begin
        tiles = (span + TILE - 1) // TILE

        m_ref[...] = jnp.full_like(m_ref, -1e30)
        l_ref[...] = jnp.zeros_like(l_ref)
        a_ref[...] = jnp.zeros_like(a_ref)
        qv = q_ref[0]
        qs = jnp.concatenate(
            [qv[:, h * HEAD_WIDTH : (h + 1) * HEAD_WIDTH] for h in range(heads)], axis=0
        )

        def tile(t, masked):
            at = begin // chunk + t * (TILE // chunk)
            kf = k_all.reshape((blocks + 1) * CORES * n_x, chunk, HEAD_WIDTH)
            vf = v_all.reshape((blocks + 1) * CORES * n_x, chunk, HEAD_WIDTH)
            kt = kf[pl.ds(at, TILE // chunk)].reshape(TILE, HEAD_WIDTH)
            vt = vf[pl.ds(at, TILE // chunk)].reshape(TILE, HEAD_WIDTH)
            s = lax.dot_general(qs, kt, (((1,), (1,)), ((), ())), preferred_element_type=jnp.float32)
            if masked:
                col = lax.broadcasted_iota(jnp.int32, (rows, TILE), 1) + (begin + t * TILE - first)
                row = lax.broadcasted_iota(jnp.int32, (rows, TILE), 0) & (chunk - 1)
                s = jnp.where(col <= row, s, -1e30)
            old = m_ref[...]
            new = jnp.maximum(old, jnp.max(s, axis=1, keepdims=True))
            alpha = jnp.exp2((old - new) * SCALE)
            p = [
                jnp.exp2((s[:, i : i + 128] - new) * SCALE) for i in range(0, TILE, 128)
            ]
            m_ref[...] = new
            l_ref[...] = l_ref[...] * alpha + sum(p[1:], p[0])
            pb = jnp.concatenate([x.astype(jnp.bfloat16) for x in p], axis=1)
            a_ref[...] = a_ref[...] * alpha + jnp.dot(pb, vt, preferred_element_type=jnp.float32)

        @pl.loop(0, tiles - 1)
        def _(t):
            tile(t, False)

        tile(tiles - 1, True)
        out = (a_ref[...] / jnp.sum(l_ref[...], axis=1, keepdims=True)).astype(jnp.bfloat16)
        for h in range(heads):
            o_ref[0, :, h * HEAD_WIDTH : (h + 1) * HEAD_WIDTH] = out[h * chunk : (h + 1) * chunk]

    smem = pl.BlockSpec(memory_space=pltpu.SMEM)
    hbm = pl.BlockSpec(memory_space=pltpu.HBM)
    row_spec = pl.BlockSpec((1, chunk, wide), lambda i: (i, 0, 0))
    return pl.pallas_call(
        kernel,
        grid=(blocks,),
        in_specs=[smem, smem, row_spec] + [hbm] * n,
        out_specs=row_spec,
        out_shape=jax.ShapeDtypeStruct(q.shape, jnp.bfloat16),
        scratch_shapes=[
            pltpu.VMEM((blocks + 1, CORES, n_x, chunk, HEAD_WIDTH), jnp.bfloat16),
            pltpu.VMEM((blocks + 1, CORES, n_x, chunk, HEAD_WIDTH), jnp.bfloat16),
            pltpu.VMEM((rows, HEAD_WIDTH), jnp.float32),
            pltpu.VMEM((rows, HEAD_WIDTH), jnp.float32),
            pltpu.VMEM((rows, HEAD_WIDTH), jnp.float32),
            pltpu.SemaphoreType.DMA((2, n)),
        ],
        compiler_params=pltpu.CompilerParams(dimension_semantics=("arbitrary",)),
    )(places, docs, q, *arrays)


def solution(mesh):
    parts, n_x, blk = mesh.devices.shape
    n_y = blk // CORES
    fine = Mesh(mesh.devices.reshape(parts, n_x, n_y, CORES), ("parts", "uly", "y", "core"))
    swap = [(2 * x + c, 2 * x + 1 - c) for x in range(n_x) for c in range(CORES)]
    ring = [
        (2 * x + c, 2 * ((x + 1 - 2 * c) % n_x) + c) for x in range(n_x) for c in range(CORES)
    ]

    def on_device(queries, keys, values, doc_blocks):
        x = lax.axis_index("uly")
        core = lax.axis_index("core")
        chunk = queries.shape[1]

        def by_head(a, wide):
            return jnp.transpose(a[0].reshape(chunk, n_y, wide), (1, 0, 2))

        kv = jnp.stack([by_head(keys, HEAD_WIDTH), by_head(values, HEAD_WIDTH)], axis=1)
        mine = lax.all_to_all(kv, "y", 0, 0, tiled=True)
        q = lax.all_to_all(by_head(queries, queries.shape[2] // n_y), "y", 0, 0, tiled=True)

        def step(a):
            return lax.ppermute(a, ("uly", "core"), ring)

        def other_core(a):
            return lax.ppermute(a, ("uly", "core"), swap)

        way = 1 - 2 * core
        other = other_core(mine)
        pieces = [(mine, x, core), (other, x, 1 - core)]
        m, o = mine, other
        for k in range(1, n_x // 2 + 1):
            here = (x - way * k) % n_x
            there = (x + way * k) % n_x
            m = step(m)
            pieces += [(m, here, core), (other_core(m), there, 1 - core)]
            if k < n_x // 2:
                o = step(o)
                pieces += [(o, here, 1 - core), (other_core(o), there, core)]
        where = jnp.stack([x, core] + [i for p in pieces for i in p[1:]]).astype(jnp.int32)
        heads = attention(where, doc_blocks, q, pieces)
        back = lax.all_to_all(heads, "y", 0, 0, tiled=True)
        return jnp.transpose(back, (1, 0, 2)).reshape(1, chunk, queries.shape[2])

    return jax.shard_map(
        on_device,
        mesh=fine,
        in_specs=(
            P(("parts", "y", "core"), "uly", None),
            P(("parts", "y", "core"), "uly", None),
            P(("parts", "y", "core"), "uly", None),
            P("parts"),
        ),
        out_specs=P(("parts", "y", "core"), "uly", None),
        check_vma=False,
    )
```

```python
import jax
import jax.numpy as jnp
from jax import lax
from jax.experimental import pallas as pl
from jax.experimental.pallas import tpu as pltpu
from jax.sharding import Mesh, PartitionSpec as P


HEAD_WIDTH = 128
BLOCK = 128
CORES = 2
TILE = 1024
SPLIT = 2
LATE = 0
VMEM_LIMIT = 32 << 20
LOG2E = 1.4426950408889634
SCALE = LOG2E * HEAD_WIDTH ** -0.5


def in_vmem(a):
    return pltpu.with_memory_space_constraint(a, pltpu.VMEM)


def in_hbm(a):
    return pltpu.with_memory_space_constraint(a, pltpu.HBM)


def attention(docs, q, pieces):
    blocks, chunk, wide = q.shape
    heads = wide // HEAD_WIDTH
    rows = heads * chunk
    arrays = [p[0] for p in pieces]
    n = len(arrays)
    n_x = n // CORES
    block_tokens = n_x * chunk
    total = blocks * CORES * block_tokens
    n_docs = docs.shape[0]
    part = rows // SPLIT

    def kernel(doc, q_ref, *refs):
        srcs, (o_ref, k_all, v_all, q_s, m_ref, a_ref, sems) = refs[:n], refs[n:]
        x = lax.axis_index("uly")
        core = lax.axis_index("core")
        way = 1 - 2 * core
        k_pieces = k_all.reshape(blocks + TILE // (CORES * block_tokens), CORES, n_x, chunk, HEAD_WIDTH)
        v_pieces = v_all.reshape(blocks + TILE // (CORES * block_tokens), CORES, n_x, chunk, HEAD_WIDTH)
        copies = []
        for i in range(n):
            at = (x - way * pieces[i][1]) % n_x
            of = core + pieces[i][2] * way
            for kind, dst in ((0, k_pieces), (1, v_pieces)):
                if i < n - LATE:
                    copies.append(
                        pltpu.make_async_copy(
                            srcs[i].at[:, kind], dst.at[pl.ds(0, blocks), of, at], sems.at[kind, i]
                        )
                    )
                    copies[-1].start()
                else:
                    for b in range(blocks):
                        dst[b, of, at] = srcs[i][b, kind]
        k_all[total:] = jnp.zeros((TILE, HEAD_WIDTH), jnp.bfloat16)
        v_all[total:] = jnp.zeros((TILE, HEAD_WIDTH), jnp.bfloat16)
        ones = jnp.ones((TILE, HEAD_WIDTH), jnp.bfloat16)
        for c in copies:
            c.wait()

        @pl.loop(0, blocks)
        def _(step):
            first = (step * CORES + core) * block_tokens + x * chunk
            begin = jnp.int32(0)
            end = jnp.int32(0)
            for i in range(n_docs):
                end = end + doc[i] * BLOCK
                begin = jnp.where(end <= first, end, begin)
            tiles = (first + chunk - begin + TILE - 1) // TILE
            for h in range(heads):
                q_s[h * chunk : (h + 1) * chunk] = q_ref[step, :, h * HEAD_WIDTH : (h + 1) * HEAD_WIDTH]
            m_ref[...] = jnp.full_like(m_ref, -1e30)
            a_ref[...] = jnp.zeros_like(a_ref)

            def tile(t, masked):
                at = pl.multiple_of(begin + t * TILE, BLOCK)
                kt = k_all[pl.ds(at, TILE)]
                vt = jnp.concatenate([v_all[pl.ds(at, TILE)], ones], axis=1)
                for g in range(SPLIT):
                    some = slice(g * part, (g + 1) * part)
                    s = lax.dot_general(
                        q_s[some], kt, (((1,), (1,)), ((), ())), preferred_element_type=jnp.float32
                    )
                    if masked:
                        col = lax.broadcasted_iota(jnp.int32, (part, TILE), 1) + (at - first)
                        row = lax.broadcasted_iota(jnp.int32, (part, TILE), 0) & (chunk - 1)
                        s = jnp.where(col <= row, s, -1e30)
                    old = m_ref[some]
                    new = jnp.maximum(old, jnp.max(s, axis=1, keepdims=True))
                    alpha = jnp.exp2((old - new) * SCALE)
                    m_ref[some] = new
                    p = jnp.concatenate(
                        [
                            jnp.exp2((s[:, i : i + 128] - new) * SCALE).astype(jnp.bfloat16)
                            for i in range(0, TILE, 128)
                        ],
                        axis=1,
                    )
                    d = jnp.dot(p, vt, preferred_element_type=jnp.float32)
                    for c in range(0, 2 * HEAD_WIDTH, HEAD_WIDTH):
                        here = slice(c, c + HEAD_WIDTH)
                        a_ref[some, here] = a_ref[some, here] * alpha + d[:, here]

            @pl.loop(0, tiles - 1)
            def _(t):
                tile(t, False)

            tile(tiles - 1, True)
            for h in range(heads):
                of = slice(h * chunk, (h + 1) * chunk)
                o_ref[step, :, h * HEAD_WIDTH : (h + 1) * HEAD_WIDTH] = (
                    a_ref[of, :HEAD_WIDTH] / a_ref[of, HEAD_WIDTH:]
                ).astype(jnp.bfloat16)

    smem = pl.BlockSpec(memory_space=pltpu.SMEM)
    hbm = pl.BlockSpec(memory_space=pltpu.HBM)
    vmem = pl.BlockSpec(memory_space=pltpu.VMEM)
    return pl.pallas_call(
        kernel,
        in_specs=[smem, vmem] + [hbm] * (n - LATE) + [vmem] * LATE,
        out_specs=vmem,
        out_shape=pltpu.VMEM(q.shape, jnp.bfloat16),
        scratch_shapes=[
            pltpu.VMEM((total + TILE, HEAD_WIDTH), jnp.bfloat16),
            pltpu.VMEM((total + TILE, HEAD_WIDTH), jnp.bfloat16),
            pltpu.VMEM((rows, HEAD_WIDTH), jnp.bfloat16),
            pltpu.VMEM((rows, HEAD_WIDTH), jnp.float32),
            pltpu.VMEM((rows, 2 * HEAD_WIDTH), jnp.float32),
            pltpu.SemaphoreType.DMA((2, n)),
        ],
        compiler_params=pltpu.CompilerParams(vmem_limit_bytes=VMEM_LIMIT),
    )(docs, in_vmem(q), *[in_hbm(a) for a in arrays[: n - LATE]], *[in_vmem(a) for a in arrays[n - LATE :]])


def by_head(keys, values, heads):
    chunk = keys.shape[1]

    def kernel(k_ref, v_ref, o_ref):
        for h in range(heads):
            o_ref[h, 0] = k_ref[0, :, h * HEAD_WIDTH : (h + 1) * HEAD_WIDTH]
            o_ref[h, 1] = v_ref[0, :, h * HEAD_WIDTH : (h + 1) * HEAD_WIDTH]

    vmem = pl.BlockSpec(memory_space=pltpu.VMEM)
    return pl.pallas_call(
        kernel,
        in_specs=[vmem, vmem],
        out_specs=vmem,
        out_shape=pltpu.VMEM((heads, 2, chunk, HEAD_WIDTH), keys.dtype),
    )(keys, values)


def side_by_side(a):
    groups, chunk, wide = a.shape

    def kernel(a_ref, o_ref, sems):
        copies = [
            pltpu.make_async_copy(a_ref.at[g], o_ref.at[0, :, pl.ds(g * wide, wide)], sems.at[g])
            for g in range(groups)
        ]
        for c in copies:
            c.start()
        for c in copies:
            c.wait()

    return pl.pallas_call(
        kernel,
        in_specs=[pl.BlockSpec(memory_space=pltpu.VMEM)],
        out_specs=pl.BlockSpec(memory_space=pltpu.HBM),
        out_shape=jax.ShapeDtypeStruct((1, chunk, groups * wide), a.dtype),
        scratch_shapes=[pltpu.SemaphoreType.DMA((groups,))],
    )(in_vmem(a))


def solution(mesh):
    parts, n_x, blk = mesh.devices.shape
    n_y = blk // CORES
    fine = Mesh(mesh.devices.reshape(parts, n_x, n_y, CORES), ("parts", "uly", "y", "core"))
    swap = [(2 * x + c, 2 * x + 1 - c) for x in range(n_x) for c in range(CORES)]
    ring = [
        (2 * x + c, 2 * ((x + 1 - 2 * c) % n_x) + c) for x in range(n_x) for c in range(CORES)
    ]

    def on_device(queries, keys, values, doc_blocks):
        chunk = queries.shape[1]
        wide = queries.shape[2] // n_y
        mine = lax.all_to_all(by_head(keys, values, n_y), "y", 0, 0, tiled=True)
        q = jnp.transpose(queries[0].reshape(chunk, n_y, wide), (1, 0, 2))
        q = lax.all_to_all(q, "y", 0, 0, tiled=True)

        def step(a):
            return lax.ppermute(a, ("uly", "core"), ring)

        def other_core(a):
            return lax.ppermute(a, ("uly", "core"), swap)

        other = other_core(mine)
        pieces = [(mine, 0, 0), (other, 0, 1)]
        m, o = mine, other
        for k in range(1, n_x // 2 + 1):
            m = step(m)
            pieces += [(m, k, 0), (other_core(m), -k, 1)]
            if k < n_x // 2:
                o = step(o)
                pieces += [(o, k, 1), (other_core(o), -k, 0)]
        heads = attention(doc_blocks, q, pieces)
        back = lax.all_to_all(heads, "y", 0, 0, tiled=True)
        return side_by_side(back)

    return jax.shard_map(
        on_device,
        mesh=fine,
        in_specs=(
            P(("parts", "y", "core"), "uly", None),
            P(("parts", "y", "core"), "uly", None),
            P(("parts", "y", "core"), "uly", None),
            P("parts"),
        ),
        out_specs=P(("parts", "y", "core"), "uly", None),
        check_vma=False,
    )
```

```python
import jax
import jax.numpy as jnp
from jax import lax
from jax.experimental import pallas as pl
from jax.experimental.pallas import tpu as pltpu
from jax.sharding import Mesh, PartitionSpec as P


HEAD_WIDTH = 128
BLOCK = 128
CORES = 2
EXTRA = 16
VMEM_LIMIT = 32 << 20
LOG2E = 1.4426950408889634
SCALE = LOG2E * HEAD_WIDTH ** -0.5


def in_vmem(a):
    return pltpu.with_memory_space_constraint(a, pltpu.VMEM)


def in_hbm(a):
    return pltpu.with_memory_space_constraint(a, pltpu.HBM)


def attention(docs, q, pieces):
    blocks, chunk, wide = q.shape
    heads = wide // HEAD_WIDTH
    rows = heads * chunk
    arrays = [p[0] for p in pieces]
    n = len(arrays)
    n_x = n // CORES
    tile = n_x * chunk
    n_docs = docs.shape[0]

    def kernel(doc, q_ref, *refs):
        srcs, (o_ref, kv, q_t, p_buf, a_ref, m_ref, bad_ref, sems) = refs[:n], refs[n:]
        x = lax.axis_index("uly")
        core = lax.axis_index("core")
        way = 1 - 2 * core
        copies = [
            pltpu.make_async_copy(
                srcs[i],
                kv.at[core + pieces[i][2] * way, (x - way * pieces[i][1]) % n_x],
                sems.at[i],
            )
            for i in range(n)
        ]
        for c in copies:
            c.start()
        bad_ref[...] = jnp.zeros_like(bad_ref)
        ones = jnp.ones((EXTRA, tile), jnp.bfloat16)

        def load(j, kind):
            return jnp.concatenate(
                [kv[lax.rem(j, CORES), a, lax.div(j, CORES), kind] for a in range(n_x)], axis=0
            )

        def span(step):
            last = step * CORES + core
            first = last * tile + x * chunk
            begin = jnp.int32(0)
            end = jnp.int32(0)
            for i in range(n_docs):
                end = end + doc[i] * BLOCK
                begin = jnp.where(end <= first, end, begin)
            return last, first, begin, lax.div(begin, tile)

        def prepare(step):
            qs = jnp.concatenate(
                [q_ref[step, :, h * HEAD_WIDTH : (h + 1) * HEAD_WIDTH] for h in range(heads)], axis=0
            )
            qf = jnp.transpose(qs.astype(jnp.float32) * SCALE)
            high = qf.astype(jnp.bfloat16)
            q_t[step & 1, :HEAD_WIDTH] = high
            q_t[step & 1, HEAD_WIDTH:] = (qf - high.astype(jnp.float32)).astype(jnp.bfloat16)

        def scores(step, j):
            kt = load(j, 0)
            return jnp.dot(
                jnp.concatenate([kt, kt], axis=1), q_t[step & 1], preferred_element_type=jnp.float32
            )

        def values(j, begin):
            vt = jnp.concatenate([jnp.transpose(load(j, 1)), ones], axis=0)
            at = lax.broadcasted_iota(jnp.int32, (1, tile), 1) + j * tile
            return vt * (at >= begin).astype(jnp.float32).astype(jnp.bfloat16)

        def allowed(j, first, begin):
            key = lax.broadcasted_iota(jnp.int32, (tile, rows), 0) + j * tile
            row = (lax.broadcasted_iota(jnp.int32, (tile, rows), 1) & (chunk - 1)) + first
            return (key <= row) & (key >= begin)

        def finish(step):
            out = a_ref[:HEAD_WIDTH] * (1.0 / a_ref[HEAD_WIDTH : HEAD_WIDTH + 1])
            out = jnp.transpose(out).astype(jnp.bfloat16)
            for h in range(heads):
                o_ref[step, :, h * HEAD_WIDTH : (h + 1) * HEAD_WIDTH] = out[
                    h * chunk : (h + 1) * chunk
                ]

        prepare(0)
        for c in copies:
            c.wait()

        @pl.loop(0, blocks)
        def _(step):
            last, first, begin, lowest = span(step)
            s = jnp.where(allowed(last, first, begin), scores(step, last), -1e30)
            top = jnp.max(s, axis=0, keepdims=True)
            m_ref[:1] = top
            p_buf[0] = jnp.exp2(s - top).astype(jnp.bfloat16)
            a_ref[...] = jnp.zeros_like(a_ref)

            def weights(j):
                return jnp.exp2(scores(step, j) - m_ref[:1]).astype(jnp.bfloat16)

            def product(j, slot):
                return jnp.dot(
                    values(j, begin), p_buf[slot], preferred_element_type=jnp.float32
                )

            count = last - lowest

            @pl.loop(0, lax.div(count, 2))
            def _(h):
                j = last - 2 * h
                p1 = weights(j - 1)
                a0 = product(j, 0)
                p2 = weights(j - 2)
                p_buf[1] = p1
                a1 = product(j - 1, 1)
                a_ref[...] += a0 + a1
                p_buf[0] = p2

            @pl.when(lax.rem(count, 2) == 1)
            def _():
                p1 = weights(lowest)
                a_ref[...] += product(lowest + 1, 0)
                p_buf[0] = p1

            a_ref[...] += product(lowest, 0)
            total = a_ref[HEAD_WIDTH : HEAD_WIDTH + 1]
            bad_ref[:1] = jnp.maximum(bad_ref[:1], jnp.where(total < 1e30, 0.0, 1.0))
            prepare(jnp.minimum(step + 1, blocks - 1))
            finish(step)

        @pl.when(jnp.max(bad_ref[...]) > 0.0)
        def _():
            @pl.loop(0, blocks)
            def _(step):
                last, first, begin, lowest = span(step)
                prepare(step)
                m_ref[...] = jnp.full_like(m_ref, -1e30)
                a_ref[...] = jnp.zeros_like(a_ref)

                @pl.loop(lowest, last + 1)
                def _(j):
                    s = jnp.where(allowed(j, first, begin), scores(step, j), -1e30)
                    old = m_ref[:1]
                    top = jnp.maximum(old, jnp.max(s, axis=0, keepdims=True))
                    m_ref[:1] = top
                    p = jnp.exp2(s - top).astype(jnp.bfloat16)
                    a_ref[...] = a_ref[...] * jnp.exp2(old - top) + jnp.dot(
                        values(j, begin), p, preferred_element_type=jnp.float32
                    )

                finish(step)

    smem = pl.BlockSpec(memory_space=pltpu.SMEM)
    hbm = pl.BlockSpec(memory_space=pltpu.HBM)
    vmem = pl.BlockSpec(memory_space=pltpu.VMEM)
    return pl.pallas_call(
        kernel,
        in_specs=[smem, vmem] + [hbm] * n,
        out_specs=vmem,
        out_shape=pltpu.VMEM(q.shape, jnp.bfloat16),
        scratch_shapes=[
            pltpu.VMEM((CORES, n_x, blocks, 2, chunk, HEAD_WIDTH), jnp.bfloat16),
            pltpu.VMEM((2, 2 * HEAD_WIDTH, rows), jnp.bfloat16),
            pltpu.VMEM((2, tile, rows), jnp.bfloat16),
            pltpu.VMEM((HEAD_WIDTH + EXTRA, rows), jnp.float32),
            pltpu.VMEM((8, rows), jnp.float32),
            pltpu.VMEM((8, rows), jnp.float32),
            pltpu.SemaphoreType.DMA((n,)),
        ],
        compiler_params=pltpu.CompilerParams(vmem_limit_bytes=VMEM_LIMIT),
    )(docs, in_vmem(q), *[in_hbm(a) for a in arrays])


def by_head(keys, values, heads):
    chunk = keys.shape[1]

    def kernel(k_ref, v_ref, o_ref):
        for h in range(heads):
            o_ref[h, 0] = k_ref[0, :, h * HEAD_WIDTH : (h + 1) * HEAD_WIDTH]
            o_ref[h, 1] = v_ref[0, :, h * HEAD_WIDTH : (h + 1) * HEAD_WIDTH]

    vmem = pl.BlockSpec(memory_space=pltpu.VMEM)
    return pl.pallas_call(
        kernel,
        in_specs=[vmem, vmem],
        out_specs=vmem,
        out_shape=pltpu.VMEM((heads, 2, chunk, HEAD_WIDTH), keys.dtype),
    )(keys, values)


def side_by_side(a):
    groups, chunk, wide = a.shape

    def kernel(a_ref, o_ref, sems):
        copies = [
            pltpu.make_async_copy(a_ref.at[g], o_ref.at[0, :, pl.ds(g * wide, wide)], sems.at[g])
            for g in range(groups)
        ]
        for c in copies:
            c.start()
        for c in copies:
            c.wait()

    return pl.pallas_call(
        kernel,
        in_specs=[pl.BlockSpec(memory_space=pltpu.VMEM)],
        out_specs=pl.BlockSpec(memory_space=pltpu.HBM),
        out_shape=jax.ShapeDtypeStruct((1, chunk, groups * wide), a.dtype),
        scratch_shapes=[pltpu.SemaphoreType.DMA((groups,))],
    )(in_vmem(a))


def solution(mesh):
    parts, n_x, blk = mesh.devices.shape
    n_y = blk // CORES
    fine = Mesh(mesh.devices.reshape(parts, n_x, n_y, CORES), ("parts", "uly", "y", "core"))
    swap = [(2 * x + c, 2 * x + 1 - c) for x in range(n_x) for c in range(CORES)]
    ring = [
        (2 * x + c, 2 * ((x + 1 - 2 * c) % n_x) + c) for x in range(n_x) for c in range(CORES)
    ]

    def on_device(queries, keys, values, doc_blocks):
        chunk = queries.shape[1]
        wide = queries.shape[2] // n_y
        mine = lax.all_to_all(by_head(keys, values, n_y), "y", 0, 0, tiled=True)
        q = jnp.transpose(queries[0].reshape(chunk, n_y, wide), (1, 0, 2))
        q = lax.all_to_all(q, "y", 0, 0, tiled=True)

        def step(a):
            return lax.ppermute(a, ("uly", "core"), ring)

        def other_core(a):
            return lax.ppermute(a, ("uly", "core"), swap)

        other = other_core(mine)
        pieces = [(mine, 0, 0), (other, 0, 1)]
        m, o = mine, other
        for k in range(1, n_x // 2 + 1):
            m = step(m)
            pieces += [(m, k, 0), (other_core(m), -k, 1)]
            if k < n_x // 2:
                o = step(o)
                pieces += [(o, k, 1), (other_core(o), -k, 0)]
        heads = attention(doc_blocks, q, pieces)
        back = lax.all_to_all(heads, "y", 0, 0, tiled=True)
        return side_by_side(back)

    return jax.shard_map(
        on_device,
        mesh=fine,
        in_specs=(
            P(("parts", "y", "core"), "uly", None),
            P(("parts", "y", "core"), "uly", None),
            P(("parts", "y", "core"), "uly", None),
            P("parts"),
        ),
        out_specs=P(("parts", "y", "core"), "uly", None),
        check_vma=False,
    )
```
